32 devices in a mesh: parts: 2 (over y), row: 16 (over z, x, core).
Axes of the slice: x: 2, y: 2, z: 4, core: 2. Of those that a mesh axis runs over, the one named last changes fastest.
Arguments:
- tokens: bfloat16 [64, 256, 768], P(('parts', 'row')), parts along dimension 0, may hold values from -6 to 6
- w_query: bfloat16 [768, 768], replicated, may hold values from -0.21875 to 0.21875
- w_key: bfloat16 [768, 768], replicated, may hold values from -0.21875 to 0.21875
- w_value: bfloat16 [768, 768], replicated, may hold values from -0.21875 to 0.21875
- w_out: bfloat16 [768, 768], replicated, may hold values from -0.21875 to 0.21875
- omega: bfloat16 [12, 64, 256], replicated, may hold values from -5 to 5
- conv_kernel: float32 [3, 3, 768], replicated, may hold values from -0.6 to 0.6
- norm_gain: float32 [768], replicated, may hold values from 0.1 to 1.9
Outputs:
- layer_out: bfloat16 [64, 256, 768], P(('parts', 'row')), parts along dimension 0
The draws below stay inside these ranges and needn't reach their ends.
There are 2 independent parts, one for each index of `parts`. The reference program is written for one: setup_inputs(seed, part) draws one part's arguments, and reference() takes and returns one part's arrays. A program takes and returns all parts, laid end to end along the dimension named above; an argument that names none is the same for every part. Nothing has to cross between parts.
All inputs are finite; a program needn't handle non-finite values.
Results may differ from the reference program's by a relative error of at most 0.0081.
Values may be sent and summed in bfloat16 or wider, within the bound.
A program may use at most 64 MiB of HBM per device.

```python
import jax
import jax.numpy as jnp
from jax import lax

D = 768
HEADS = 12
DH = 64
FEAT = 256
COLS = 256
ROWS_DEV = 2
GRID_ROWS = 32


def block_scale(stream_key, shape, split, low, high):
    def one(dim, shards_of):
        heights = jax.random.uniform(jax.random.fold_in(jax.random.fold_in(stream_key, 6), dim), (shards_of,), jnp.float32, low / len(split), high / len(split))
        return jnp.repeat(jnp.exp(heights), shape[dim] // shards_of).reshape((-1,) + (1,) * (len(shape) - dim - 1))

    factor_of = one(*split[0])
    for cut in split[1:]:
        factor_of = factor_of * one(*cut)
    return factor_of


def centred(stream_key, dims, scale, bound, shards=(), held_as=jnp.bfloat16):
    gain = block_scale(stream_key, dims, shards, -0.22, 0.18) if shards else 1.0
    values = jax.random.normal(stream_key, dims, jnp.float32) * scale * gain
    return jnp.minimum(jnp.maximum(values, -bound), bound).astype(held_as)


def setup_inputs(seed: int = 0, part: int = 0) -> dict:
    streams_of = jax.random.split(jax.random.key(seed), 9)
    own_keys = jax.random.split(jax.random.fold_in(streams_of[8], part), 9)
    tokens = centred(own_keys[0], (GRID_ROWS, COLS, D), 1.0, 6.0, ((0, 16),))
    w_query = centred(streams_of[1], (D, D), D ** -0.5, 0.21875)
    w_key = centred(streams_of[2], (D, D), D ** -0.5, 0.21875)
    w_value = centred(streams_of[3], (D, D), D ** -0.5, 0.21875)
    w_out = centred(streams_of[4], (D, D), D ** -0.5, 0.21875)
    omega = centred(streams_of[5], (HEADS, DH, FEAT), 1.0, 5.0)
    conv_kernel = jnp.clip(jax.random.uniform(streams_of[6], (3, 3, D), jnp.float32, -0.6, 0.6), -0.6, 0.6)
    norm_gain = jnp.clip(1.0 + 0.18 * jax.random.normal(streams_of[7], (D,), jnp.float32), 0.1, 1.9)
    return {"tokens": tokens, "w_query": w_query, "w_key": w_key, "w_value": w_value, "w_out": w_out, "omega": omega, "conv_kernel": conv_kernel, "norm_gain": norm_gain}


def project(rows, weight):
    return jnp.dot(rows, weight, preferred_element_type=jnp.float32).astype(jnp.bfloat16)

def feature_map(heads_in, omega):
    dim_head = heads_in.shape[-1]
    values = heads_in.astype(jnp.float32)
    lifted = jnp.einsum('thd,hdf->thf', values, omega.astype(jnp.float32))
    square = lax.optimization_barrier(jnp.sum(values * values, axis=-1, keepdims=True))
    feats = jnp.exp(lifted * dim_head ** (-0.25) - square * 0.5 * dim_head ** (-0.5)) * omega.shape[-1] ** (-0.5)
    return feats.astype(jnp.bfloat16)

def reference(tokens, w_query, w_key, w_value, w_out, omega, conv_kernel, norm_gain):
    grid_rows, cols, width = tokens.shape
    heads, dim_head, nfeat = omega.shape
    blocks = grid_rows // ROWS_DEV
    flat = tokens.reshape(grid_rows * cols, width)
    value = project(flat, w_value)
    value_blocks = value.reshape(blocks, ROWS_DEV * cols, heads, dim_head)
    token_blocks = tokens.reshape(blocks, ROWS_DEV * cols, width)

    def add_state(carry, pair):
        rows, vals = pair
        feat_key = feature_map(project(rows, w_key).reshape(-1, heads, dim_head), omega).astype(jnp.float32)
        state = carry[0] + jnp.einsum('thf,thd->fhd', feat_key, vals.astype(jnp.float32))
        total = carry[1] + lax.optimization_barrier(jnp.sum(feat_key, axis=0)).astype(jnp.float32)
        return ((state, total), None)
    init = (jnp.zeros((nfeat, heads, dim_head), jnp.float32), jnp.zeros((heads, nfeat), jnp.float32))
    (kv_sum, key_sum), unused = lax.scan(add_state, init, (token_blocks, value_blocks))
    kv_state = kv_sum.astype(jnp.bfloat16).astype(jnp.float32)
    padded = jnp.pad(value.reshape(grid_rows, cols, width).astype(jnp.float32), ((1, 1), (1, 1), (0, 0)))
    position = jnp.zeros((grid_rows, cols, width), jnp.float32)
    for shift_a in range(3):
        for shift_b in range(3):
            position = position + padded[shift_a:shift_a + grid_rows, shift_b:shift_b + cols, :] * conv_kernel[shift_a, shift_b]
    position_blocks = position.reshape(blocks, ROWS_DEV * cols, width)

    def block_out(pair):
        rows, local_pos = pair
        feat_query = feature_map(project(rows, w_query).reshape(-1, heads, dim_head), omega).astype(jnp.float32)
        numer = jnp.einsum('thf,fhd->thd', feat_query, kv_state, precision=lax.Precision.HIGHEST)
        denom = jnp.einsum('thf,hf->th', feat_query, key_sum, precision=lax.Precision.HIGHEST)
        attn = numer / denom[:, :, None]
        scale = lax.rsqrt(lax.optimization_barrier(jnp.mean(attn * attn, axis=(1, 2), keepdims=True)) + 1e-06)
        normed = (attn * scale).reshape(-1, width) * norm_gain
        mixed = (normed + local_pos).astype(jnp.bfloat16)
        out = rows.astype(jnp.float32) + jnp.dot(mixed, w_out, preferred_element_type=jnp.float32)
        return out.astype(jnp.bfloat16)
    outs = lax.map(block_out, (token_blocks, position_blocks))
    return outs.reshape(grid_rows, cols, width)
```

```python
import functools
import math

import jax
import jax.numpy as jnp
from jax import lax
from jax.experimental import pallas as pl
from jax.experimental.pallas import tpu as pltpu
from jax.sharding import PartitionSpec as P

F32, BF16 = jnp.float32, jnp.bfloat16
LANES, SUB = 128, 16


def with_halo(block, sides, width):
    for axis, dim in sides:
        count = lax.axis_size(axis)
        forward = [(i, i + 1) for i in range(count - 1)]
        backward = [(target, source) for source, target in forward]
        low = lax.ppermute(
            lax.slice_in_dim(block, block.shape[dim] - width, None, axis=dim), axis, forward
        )
        high = lax.ppermute(lax.slice_in_dim(block, 0, width, axis=dim), axis, backward)
        block = jnp.concatenate([low, block, high], axis=dim)
    return block


def project(rows, weight):
    return jnp.dot(rows, weight, preferred_element_type=jnp.float32).astype(jnp.bfloat16)


def feature_map(heads_in, omega):
    dim_head = heads_in.shape[-1]
    lifted = jnp.einsum("thd,hdf->thf", heads_in, omega, preferred_element_type=jnp.float32)
    values = heads_in.astype(jnp.float32)
    square = jnp.sum(values * values, axis=-1, keepdims=True)
    feats = jnp.exp(lifted * dim_head ** (-0.25) - square * 0.5 * dim_head ** (-0.5)) * omega.shape[
        -1
    ] ** (-0.5)
    return feats.astype(jnp.bfloat16)


def shards(tokens, w_query, w_key, w_value, w_out, omega, conv_kernel, norm_gain):
    rows_here, cols, width = tokens.shape
    heads, dim_head, nfeat = omega.shape
    flat = tokens.reshape(rows_here * cols, width)
    value = project(flat, w_value)
    value_ext = with_halo(value.reshape(rows_here, cols, width), (("row", 0),), 1)
    feat_key = feature_map(project(flat, w_key).reshape(-1, heads, dim_head), omega)
    local_state = jnp.einsum(
        "thf,thd->fhd",
        feat_key,
        value.reshape(-1, heads, dim_head),
        preferred_element_type=jnp.float32,
    )
    local_sum = jnp.sum(feat_key.astype(jnp.float32), axis=0)
    feat_query = feature_map(project(flat, w_query).reshape(-1, heads, dim_head), omega)
    padded = jnp.pad(value_ext.astype(jnp.float32), ((0, 0), (1, 1), (0, 0)))
    position = jnp.zeros((rows_here, cols, width), jnp.float32)
    for shift_a in range(3):
        for shift_b in range(3):
            position = (
                position
                + padded[shift_a : shift_a + rows_here, shift_b : shift_b + cols, :]
                * conv_kernel[shift_a, shift_b]
            )
    kv_sum, key_sum = lax.psum((local_state.reshape(nfeat, width), local_sum), "row")
    kv_state = kv_sum.astype(jnp.bfloat16).reshape(nfeat, heads, dim_head)
    numer = jnp.einsum("thf,fhd->thd", feat_query, kv_state, preferred_element_type=jnp.float32)
    denom = jnp.einsum(
        "thf,hf->th", feat_query.astype(jnp.float32), key_sum, precision=lax.Precision.HIGHEST
    )
    attn = numer / denom[:, :, None]
    scale = lax.rsqrt(jnp.mean(attn * attn, axis=(1, 2), keepdims=True) + 1e-06)
    normed = (attn * scale).reshape(-1, width) * norm_gain
    mixed = (normed + position.reshape(-1, width)).astype(jnp.bfloat16)
    out = flat.astype(jnp.float32) + jnp.dot(mixed, w_out, preferred_element_type=jnp.float32)
    return out.astype(jnp.bfloat16).reshape(rows_here, cols, width)


def mm(a, b):
    return jnp.dot(a, b, preferred_element_type=F32)


def kernel(
    dims,
    tok_hbm, wq_hbm, wk_hbm, wv_hbm, wo_hbm, om_hbm, conv_ref, gain_ref,
    out_hbm,
    tok, wq, wk, wv, wo, om, val, halo, fq, pos, att, outv,
    stf, kst, d2d_src, d2d_dst, rs_src, rs_dst, fin,
    load_sem, out_sem, halo_s, halo_r, d2d_s, d2d_r, rs_s, rs_r, ag_s, ag_r, fw_s, fw_r,
):
    n, rows_here, cols, width, heads, dh, nfeat, groups = dims
    chips, half = n // 2, nfeat // 2
    piece = half // chips
    pairs = heads // 2
    nrows = rows_here * cols
    me = lax.axis_index("row")
    chip, core = me // 2, me % 2
    mate = me + 1 - 2 * core

    loads = [
        pltpu.make_async_copy(src, dst, load_sem.at[i])
        for i, (src, dst) in enumerate(
            [(tok_hbm, tok), (wv_hbm, wv), (wk_hbm, wk), (om_hbm, om), (wq_hbm, wq), (wo_hbm, wo)]
        )
    ]
    for copy in loads:
        copy.start()

    barrier = pltpu.get_barrier_semaphore()
    for d in range(1, n):
        pl.semaphore_signal(
            barrier, inc=1, device_id={"row": lax.rem(me + d, n)},
            device_id_type=pl.DeviceIdType.MESH,
        )

    def remote(src, dst, s, r, target):
        return pltpu.make_async_remote_copy(
            src_ref=src, dst_ref=dst, send_sem=s, recv_sem=r,
            device_id={"row": target}, device_id_type=pl.DeviceIdType.MESH,
        )

    lane_lo = lax.broadcasted_iota(jnp.int32, (1, LANES), 1) < dh
    sq_scale = 0.5 * dh ** (-0.5) * dh ** 0.25
    arg_scale = dh ** (-0.25)
    arg_shift = 0.5 * math.log(nfeat)
    minus = jnp.full((LANES, nfeat), -1.0, BF16)
    zero_om = jnp.zeros((dh, nfeat), BF16)

    def feats(u, pair):
        uf = u.astype(F32)
        sq = uf * uf * sq_scale
        hi = sq.astype(BF16).astype(F32)
        lo = pltpu.roll(sq - hi, dh, 1)
        out = []
        for k in range(2):
            tail = jnp.where(lane_lo, hi, lo) if k == 0 else jnp.where(lane_lo, lo, hi)
            lhs = jnp.concatenate([u, tail.astype(BF16)], axis=1)
            o = om[2 * pair + k]
            top = [o, zero_om] if k == 0 else [zero_om, o]
            rhs = jnp.concatenate(top + [minus], axis=0)
            out.append(jnp.exp(mm(lhs, rhs) * arg_scale - arg_shift).astype(BF16))
        return out

    loads[0].wait()
    loads[1].wait()
    t = tok[...]
    for q in range(0, width, 2 * LANES):
        val[:, q : q + 2 * LANES] = mm(t, wv[:, q : q + 2 * LANES]).astype(BF16)
    pl.semaphore_wait(barrier, n - 1)
    to_next = remote(val.at[pl.ds(nrows - cols, cols)], halo.at[0], halo_s.at[0], halo_r.at[0],
                     lax.rem(me + 1, n))
    to_prev = remote(val.at[pl.ds(0, cols)], halo.at[1], halo_s.at[1], halo_r.at[1],
                     lax.rem(me + n - 1, n))

    @pl.when(me < n - 1)
    def _():
        to_next.start()

    @pl.when(me > 0)
    def _():
        to_prev.start()

    own_rows = pl.ds(pl.multiple_of(core * half, half), half)
    mate_rows = pl.ds(pl.multiple_of((1 - core) * half, half), half)
    d2d = [
        remote(d2d_src.at[s], d2d_dst.at[s], d2d_s.at[s], d2d_r.at[s], mate)
        for s in range(pairs + 1)
    ]

    def put_slab(s, block):
        stf[s] = block
        d2d_src[s] = stf[s, mate_rows, :].astype(BF16)
        d2d[s].start()

    kst[...] = jnp.zeros_like(kst)
    ones = jnp.ones((SUB, nrows), BF16)

    def key_quad(g):
        u2 = mm(t, wk[:, 2 * LANES * g : 2 * LANES * (g + 1)]).astype(BF16)
        for i in range(2):
            pair = 2 * g + i
            f0, f1 = feats(u2[:, LANES * i : LANES * (i + 1)], pair)
            vt = val[:, LANES * pair : LANES * (pair + 1)].T
            lhs = jnp.concatenate([vt, ones], axis=0)
            s0, s1 = mm(lhs, f0), mm(lhs, f1)
            kst[2 * pair : 2 * pair + 1, :] = s0[LANES : LANES + 1]
            kst[2 * pair + 1 : 2 * pair + 2, :] = s1[LANES : LANES + 1]
            put_slab(pair, jnp.concatenate([s0[:dh], s1[dh:LANES]], axis=0).T)

    def query_quad(g):
        u2 = mm(t, wq[:, 2 * LANES * g : 2 * LANES * (g + 1)]).astype(BF16)
        for i in range(2):
            pair = 2 * g + i
            f0, f1 = feats(u2[:, LANES * i : LANES * (i + 1)], pair)
            fq[2 * pair] = f0
            fq[2 * pair + 1] = f1

    rs, ag, fw = [], [], []
    my_rows = pl.ds(pl.multiple_of(core * half + chip * piece, piece), piece)
    for gi, (a, b) in enumerate(groups):
        rs_g, ag_g = [], []
        for d in range(1, chips):
            peer = lax.rem(chip + d, chips)
            rs_g.append(remote(rs_src.at[peer, a:b], rs_dst.at[d, a:b],
                               rs_s.at[gi, d], rs_r.at[gi, d], 2 * peer + core))
            ag_g.append(remote(fin.at[a:b, my_rows], fin.at[a:b, my_rows],
                               ag_s.at[gi, d], ag_r.at[gi, d], 2 * peer + core))
        rs.append(rs_g)
        ag.append(ag_g)
        fw_g = []
        for d in range(chips):
            source = lax.rem(chip + chips - d, chips)
            rows = pl.ds(pl.multiple_of(core * half + source * piece, piece), piece)
            fw_g.append(remote(fin.at[a:b, rows], fin.at[a:b, rows],
                               fw_s.at[gi, d], fw_r.at[gi, d], mate))
        fw.append(fw_g)

    def scatter(gi):
        a, b = groups[gi]
        for s in range(a, b):
            d2d[s].wait_recv()
            both = stf[s, own_rows, :] + d2d_dst[s].astype(F32)
            rs_src[:, s] = both.astype(BF16).reshape(chips, piece, LANES)
        for copy in reversed(rs[gi]):
            copy.start()

    def gather(gi):
        a, b = groups[gi]
        total = rs_src[chip, a:b].astype(F32)
        for d in range(1, chips):
            rs[gi][d - 1].wait_recv()
            total = total + rs_dst[d, a:b].astype(F32)
        fin[a:b, my_rows, :] = total.astype(BF16)
        for copy in reversed(ag[gi]):
            copy.start()
        fw[gi][0].start()

    def forward(gi):
        for d in range(1, chips):
            ag[gi][d - 1].wait_recv()
            fw[gi][d].start()

    def convolve():
        @pl.when(me < n - 1)
        def _():
            to_prev.wait_recv()

        @pl.when(me > 0)
        def _():
            to_next.wait_recv()

        @pl.when(me == n - 1)
        def _():
            halo[1] = jnp.zeros_like(halo[1])

        @pl.when(me == 0)
        def _():
            halo[0] = jnp.zeros_like(halo[0])

        col = lax.broadcasted_iota(jnp.int32, (cols, LANES), 0)
        for q in range(0, width, LANES):
            cut = slice(q, q + LANES)
            lines = [halo[0, :, cut]]
            lines += [val[r * cols : (r + 1) * cols, cut] for r in range(rows_here)]
            lines += [halo[1, :, cut]]
            lines = [x.astype(F32) for x in lines]
            for r in range(rows_here):
                acc = []
                for b in range(3):
                    part = lines[r] * conv_ref[0, b : b + 1, cut]
                    for a in range(1, 3):
                        part = part + lines[r + a] * conv_ref[a, b : b + 1, cut]
                    acc.append(part)
                left = jnp.where(col == 0, 0.0, pltpu.roll(acc[0], 1, 0))
                right = jnp.where(col == cols - 1, 0.0, pltpu.roll(acc[2], cols - 1, 0))
                pos[r * cols : (r + 1) * cols, cut] = acc[1] + left + right

    loads[2].wait()
    loads[3].wait()
    key_quad(0)
    key_quad(1)
    scatter(0)
    key_quad(2)
    put_slab(pairs, kst[...].T)
    loads[4].wait()
    query_quad(0)
    scatter(1)
    query_quad(1)
    gather(0)
    query_quad(2)
    gather(1)
    convolve()
    forward(0)
    forward(1)
    for gi in range(len(groups)):
        for copy in fw[gi]:
            copy.wait_recv()

    ks = fin[pairs]
    sumsq = jnp.zeros((nrows, LANES), F32)
    pick_row = lax.broadcasted_iota(jnp.int32, (LANES, LANES), 0)
    pick_lane = lax.broadcasted_iota(jnp.int32, (LANES, LANES), 1) // dh
    zero = jnp.zeros((), BF16)
    for p in range(pairs):
        pick = jnp.where(pick_row == 2 * p + pick_lane, 1.0, 0.0).astype(BF16)
        krep = mm(ks, pick).astype(BF16)
        sp = fin[p]
        lo = jnp.concatenate([jnp.where(lane_lo, sp, zero), jnp.where(lane_lo, krep, zero)], 1)
        hi = jnp.concatenate([jnp.where(lane_lo, zero, sp), jnp.where(lane_lo, zero, krep)], 1)
        both = mm(fq[2 * p], lo) + mm(fq[2 * p + 1], hi)
        attn = both[:, :LANES] / both[:, LANES:]
        att[:, LANES * p : LANES * (p + 1)] = attn
        sumsq = sumsq + attn * attn
    scale = lax.rsqrt(jnp.sum(sumsq, axis=1, keepdims=True) * (1.0 / width) + 1e-06)
    loads[5].wait()
    outs = []
    for r in range(rows_here):
        cut = slice(r * cols, (r + 1) * cols)
        mixed = (att[cut] * scale[cut] * gain_ref[...] + pos[cut]).astype(BF16)
        outv[cut] = (tok[cut].astype(F32) + mm(mixed, wo[...])).astype(BF16)
        copy = pltpu.make_async_copy(outv.at[cut], out_hbm.at[cut], out_sem.at[r])
        copy.start()
        outs.append(copy)

    @pl.when(me < n - 1)
    def _():
        to_next.wait_send()

    @pl.when(me > 0)
    def _():
        to_prev.wait_send()

    for copy in d2d:
        copy.wait_send()
    for gi in range(len(groups)):
        for copy in rs[gi] + ag[gi] + fw[gi]:
            copy.wait_send()
    for copy in outs:
        copy.wait()


def fused(n, tokens, w_query, w_key, w_value, w_out, omega, conv_kernel, norm_gain):
    rows_here, cols, width = tokens.shape
    heads, dh, nfeat = omega.shape
    nrows = rows_here * cols
    chips, half, slabs = n // 2, nfeat // 2, heads // 2 + 1
    piece = half // chips
    groups = ((0, 4), (4, slabs))
    dims = (n, rows_here, cols, width, heads, dh, nfeat, groups)
    any_spec = pl.BlockSpec(memory_space=pl.ANY)
    vmem_spec = pl.BlockSpec(memory_space=pltpu.VMEM)
    sem = pltpu.SemaphoreType.DMA
    ng = len(groups)
    flat = tokens.reshape(nrows, width)
    out = pl.pallas_call(
        functools.partial(kernel, dims),
        out_shape=jax.ShapeDtypeStruct((nrows, width), BF16),
        in_specs=[any_spec] * 6 + [vmem_spec] * 2,
        out_specs=any_spec,
        scratch_shapes=[
            pltpu.VMEM((nrows, width), BF16),
            pltpu.VMEM((width, width), BF16),
            pltpu.VMEM((width, width), BF16),
            pltpu.VMEM((width, width), BF16),
            pltpu.VMEM((width, width), BF16),
            pltpu.VMEM((heads, dh, nfeat), BF16),
            pltpu.VMEM((nrows, width), BF16),
            pltpu.VMEM((2, cols, width), BF16),
            pltpu.VMEM((heads, nrows, nfeat), BF16),
            pltpu.VMEM((nrows, width), F32),
            pltpu.VMEM((nrows, width), F32),
            pltpu.VMEM((nrows, width), BF16),
            pltpu.VMEM((slabs, nfeat, LANES), F32),
            pltpu.VMEM((LANES, nfeat), F32),
            pltpu.VMEM((slabs, half, LANES), BF16),
            pltpu.VMEM((slabs, half, LANES), BF16),
            pltpu.VMEM((chips, slabs, piece, LANES), BF16),
            pltpu.VMEM((chips, slabs, piece, LANES), BF16),
            pltpu.VMEM((slabs, nfeat, LANES), BF16),
            sem((6,)), sem((rows_here,)), sem((2,)), sem((2,)), sem((slabs,)), sem((slabs,)),
            sem((ng, chips)), sem((ng, chips)), sem((ng, chips)), sem((ng, chips)),
            sem((ng, chips)), sem((ng, chips)),
        ],
        compiler_params=pltpu.CompilerParams(
            collective_id=0, has_side_effects=True, vmem_limit_bytes=60 * 1024 * 1024
        ),
    )(flat, w_query, w_key, w_value, w_out, omega, conv_kernel, norm_gain.reshape(1, width))
    return out.reshape(tokens.shape)


def layer(n, *args):
    heads, dh, nfeat = args[5].shape
    width = args[0].shape[2]
    fits = (
        n % 2 == 0 and nfeat % (n * SUB) == 0 and 2 * dh == LANES and heads == 12
        and nfeat == 2 * LANES and width == heads * dh
    )
    return fused(n, *args) if fits else shards(*args)


def solution(mesh):
    return jax.shard_map(
        functools.partial(layer, mesh.shape["row"]),
        mesh=mesh,
        in_specs=(P(("parts", "row"), None, None), P(), P(), P(), P(), P(), P(), P()),
        out_specs=P(("parts", "row"), None, None),
        check_vma=False,
    )
```

```python
import functools
import math

import jax
import jax.numpy as jnp
from jax import lax
from jax.experimental import pallas as pl
from jax.experimental.pallas import tpu as pltpu
from jax.sharding import PartitionSpec as P

F32, BF16 = jnp.float32, jnp.bfloat16
LANES, SUB = 128, 16


def with_halo(block, sides, width):
    for axis, dim in sides:
        count = lax.axis_size(axis)
        forward = [(i, i + 1) for i in range(count - 1)]
        backward = [(target, source) for source, target in forward]
        low = lax.ppermute(
            lax.slice_in_dim(block, block.shape[dim] - width, None, axis=dim), axis, forward
        )
        high = lax.ppermute(lax.slice_in_dim(block, 0, width, axis=dim), axis, backward)
        block = jnp.concatenate([low, block, high], axis=dim)
    return block


def project(rows, weight):
    return jnp.dot(rows, weight, preferred_element_type=jnp.float32).astype(jnp.bfloat16)


def feature_map(heads_in, omega):
    dim_head = heads_in.shape[-1]
    lifted = jnp.einsum("thd,hdf->thf", heads_in, omega, preferred_element_type=jnp.float32)
    values = heads_in.astype(jnp.float32)
    square = jnp.sum(values * values, axis=-1, keepdims=True)
    feats = jnp.exp(lifted * dim_head ** (-0.25) - square * 0.5 * dim_head ** (-0.5)) * omega.shape[
        -1
    ] ** (-0.5)
    return feats.astype(jnp.bfloat16)


def shards(tokens, w_query, w_key, w_value, w_out, omega, conv_kernel, norm_gain):
    rows_here, cols, width = tokens.shape
    heads, dim_head, nfeat = omega.shape
    flat = tokens.reshape(rows_here * cols, width)
    value = project(flat, w_value)
    value_ext = with_halo(value.reshape(rows_here, cols, width), (("row", 0),), 1)
    feat_key = feature_map(project(flat, w_key).reshape(-1, heads, dim_head), omega)
    local_state = jnp.einsum(
        "thf,thd->fhd",
        feat_key,
        value.reshape(-1, heads, dim_head),
        preferred_element_type=jnp.float32,
    )
    local_sum = jnp.sum(feat_key.astype(jnp.float32), axis=0)
    feat_query = feature_map(project(flat, w_query).reshape(-1, heads, dim_head), omega)
    padded = jnp.pad(value_ext.astype(jnp.float32), ((0, 0), (1, 1), (0, 0)))
    position = jnp.zeros((rows_here, cols, width), jnp.float32)
    for shift_a in range(3):
        for shift_b in range(3):
            position = (
                position
                + padded[shift_a : shift_a + rows_here, shift_b : shift_b + cols, :]
                * conv_kernel[shift_a, shift_b]
            )
    kv_sum, key_sum = lax.psum((local_state.reshape(nfeat, width), local_sum), "row")
    kv_state = kv_sum.astype(jnp.bfloat16).reshape(nfeat, heads, dim_head)
    numer = jnp.einsum("thf,fhd->thd", feat_query, kv_state, preferred_element_type=jnp.float32)
    denom = jnp.einsum(
        "thf,hf->th", feat_query.astype(jnp.float32), key_sum, precision=lax.Precision.HIGHEST
    )
    attn = numer / denom[:, :, None]
    scale = lax.rsqrt(jnp.mean(attn * attn, axis=(1, 2), keepdims=True) + 1e-06)
    normed = (attn * scale).reshape(-1, width) * norm_gain
    mixed = (normed + position.reshape(-1, width)).astype(jnp.bfloat16)
    out = flat.astype(jnp.float32) + jnp.dot(mixed, w_out, preferred_element_type=jnp.float32)
    return out.astype(jnp.bfloat16).reshape(rows_here, cols, width)


def mm(a, b):
    return jnp.dot(a, b, preferred_element_type=F32)


def kernel(
    dims,
    tok_hbm, wq_hbm, wk_hbm, wv_hbm, wo_hbm, om_hbm, conv_ref, gain_ref,
    out_hbm,
    tok, wq, wk, wv, wo, om, val, halo, fq, pos, att, outv,
    stf, kst, d2d_src, d2d_dst, rs_src, rs_dst, fin,
    load_sem, out_sem, halo_s, halo_r, d2d_s, d2d_r, rs_s, rs_r, ag_s, ag_r, fw_s, fw_r,
):
    n, rows_here, cols, width, heads, dh, nfeat, groups = dims
    chips, half = n // 2, nfeat // 2
    piece = half // chips
    pairs = heads // 2
    nrows = rows_here * cols
    me = lax.axis_index("row")
    chip, core = me // 2, me % 2
    mate = me + 1 - 2 * core

    loads = [
        pltpu.make_async_copy(src, dst, load_sem.at[i])
        for i, (src, dst) in enumerate(
            [(tok_hbm, tok), (wv_hbm, wv), (wk_hbm, wk), (om_hbm, om), (wq_hbm, wq), (wo_hbm, wo)]
        )
    ]
    for copy in loads:
        copy.start()

    barrier = pltpu.get_barrier_semaphore()
    for d in range(1, n):
        pl.semaphore_signal(
            barrier, inc=1, device_id={"row": lax.rem(me + d, n)},
            device_id_type=pl.DeviceIdType.MESH,
        )

    def remote(src, dst, s, r, target):
        return pltpu.make_async_remote_copy(
            src_ref=src, dst_ref=dst, send_sem=s, recv_sem=r,
            device_id={"row": target}, device_id_type=pl.DeviceIdType.MESH,
        )

    lane_lo = lax.broadcasted_iota(jnp.int32, (1, LANES), 1) < dh
    sq_scale = 0.5 * dh ** (-0.5) * dh ** 0.25
    arg_scale = dh ** (-0.25)
    arg_shift = 0.5 * math.log(nfeat)
    minus = jnp.full((LANES, nfeat), -1.0, BF16)
    zero_om = jnp.zeros((dh, nfeat), BF16)

    def feats(u, pair):
        uf = u.astype(F32)
        sq = uf * uf * sq_scale
        hi = sq.astype(BF16).astype(F32)
        lo = pltpu.roll(sq - hi, dh, 1)
        out = []
        for k in range(2):
            tail = jnp.where(lane_lo, hi, lo) if k == 0 else jnp.where(lane_lo, lo, hi)
            lhs = jnp.concatenate([u, tail.astype(BF16)], axis=1)
            o = om[2 * pair + k]
            top = [o, zero_om] if k == 0 else [zero_om, o]
            rhs = jnp.concatenate(top + [minus], axis=0)
            out.append(jnp.exp(mm(lhs, rhs) * arg_scale - arg_shift).astype(BF16))
        return out

    loads[0].wait()
    loads[1].wait()
    t = tok[...]
    for q in range(0, width, 2 * LANES):
        val[:, q : q + 2 * LANES] = mm(t, wv[:, q : q + 2 * LANES]).astype(BF16)
    pl.semaphore_wait(barrier, n - 1)
    to_next = remote(val.at[pl.ds(nrows - cols, cols)], halo.at[0], halo_s.at[0], halo_r.at[0],
                     lax.rem(me + 1, n))
    to_prev = remote(val.at[pl.ds(0, cols)], halo.at[1], halo_s.at[1], halo_r.at[1],
                     lax.rem(me + n - 1, n))

    @pl.when(me < n - 1)
    def _():
        to_next.start()

    @pl.when(me > 0)
    def _():
        to_prev.start()

    own_rows = pl.ds(pl.multiple_of(core * half, half), half)
    mate_rows = pl.ds(pl.multiple_of((1 - core) * half, half), half)
    d2d = [
        remote(d2d_src.at[s], d2d_dst.at[s], d2d_s.at[s], d2d_r.at[s], mate)
        for s in range(pairs + 1)
    ]

    def put_slab(s, block):
        stf[s] = block
        d2d_src[s] = stf[s, mate_rows, :].astype(BF16)
        d2d[s].start()

    kst[...] = jnp.zeros_like(kst)
    ones = jnp.ones((SUB, nrows), BF16)

    def key_quad(g):
        u2 = mm(t, wk[:, 2 * LANES * g : 2 * LANES * (g + 1)]).astype(BF16)
        for i in range(2):
            pair = 2 * g + i
            f0, f1 = feats(u2[:, LANES * i : LANES * (i + 1)], pair)
            vt = val[:, LANES * pair : LANES * (pair + 1)].T
            lhs = jnp.concatenate([vt, ones], axis=0)
            s0, s1 = mm(lhs, f0), mm(lhs, f1)
            kst[2 * pair : 2 * pair + 1, :] = s0[LANES : LANES + 1]
            kst[2 * pair + 1 : 2 * pair + 2, :] = s1[LANES : LANES + 1]
            put_slab(pair, jnp.concatenate([s0[:dh], s1[dh:LANES]], axis=0).T)

    def query_quad(g):
        u2 = mm(t, wq[:, 2 * LANES * g : 2 * LANES * (g + 1)]).astype(BF16)
        for i in range(2):
            pair = 2 * g + i
            f0, f1 = feats(u2[:, LANES * i : LANES * (i + 1)], pair)
            fq[2 * pair] = f0
            fq[2 * pair + 1] = f1

    rs, ag, fw = [], [], []
    my_rows = pl.ds(pl.multiple_of(core * half + chip * piece, piece), piece)
    for gi, (a, b) in enumerate(groups):
        rs_g, ag_g = [], []
        for d in range(1, chips):
            peer = lax.rem(chip + d, chips)
            rs_g.append(remote(rs_src.at[peer, a:b], rs_dst.at[d, a:b],
                               rs_s.at[gi, d], rs_r.at[gi, d], 2 * peer + core))
            ag_g.append(remote(fin.at[a:b, my_rows], fin.at[a:b, my_rows],
                               ag_s.at[gi, d], ag_r.at[gi, d], 2 * peer + core))
        rs.append(rs_g)
        ag.append(ag_g)
        fw_g = []
        for d in range(chips):
            source = lax.rem(chip + chips - d, chips)
            rows = pl.ds(pl.multiple_of(core * half + source * piece, piece), piece)
            fw_g.append(remote(fin.at[a:b, rows], fin.at[a:b, rows],
                               fw_s.at[gi, d], fw_r.at[gi, d], mate))
        fw.append(fw_g)

    def scatter(gi):
        a, b = groups[gi]
        for s in range(a, b):
            d2d[s].wait_recv()
            both = stf[s, own_rows, :] + d2d_dst[s].astype(F32)
            rs_src[:, s] = both.astype(BF16).reshape(chips, piece, LANES)
        for copy in reversed(rs[gi]):
            copy.start()

    def gather(gi):
        a, b = groups[gi]
        total = rs_src[chip, a:b].astype(F32)
        for d in range(1, chips):
            rs[gi][d - 1].wait_recv()
            total = total + rs_dst[d, a:b].astype(F32)
        fin[a:b, my_rows, :] = total.astype(BF16)
        for copy in reversed(ag[gi]):
            copy.start()
        fw[gi][0].start()

    def forward(gi):
        for d in range(1, chips):
            ag[gi][d - 1].wait_recv()
            fw[gi][d].start()

    def convolve():
        @pl.when(me < n - 1)
        def _():
            to_prev.wait_recv()

        @pl.when(me > 0)
        def _():
            to_next.wait_recv()

        @pl.when(me == n - 1)
        def _():
            halo[1] = jnp.zeros_like(halo[1])

        @pl.when(me == 0)
        def _():
            halo[0] = jnp.zeros_like(halo[0])

        col = lax.broadcasted_iota(jnp.int32, (cols, LANES), 0)
        for q in range(0, width, LANES):
            cut = slice(q, q + LANES)
            lines = [halo[0, :, cut]]
            lines += [val[r * cols : (r + 1) * cols, cut] for r in range(rows_here)]
            lines += [halo[1, :, cut]]
            lines = [x.astype(F32) for x in lines]
            for r in range(rows_here):
                acc = []
                for b in range(3):
                    part = lines[r] * conv_ref[0, b : b + 1, cut]
                    for a in range(1, 3):
                        part = part + lines[r + a] * conv_ref[a, b : b + 1, cut]
                    acc.append(part)
                left = jnp.where(col == 0, 0.0, pltpu.roll(acc[0], 1, 0))
                right = jnp.where(col == cols - 1, 0.0, pltpu.roll(acc[2], cols - 1, 0))
                pos[r * cols : (r + 1) * cols, cut] = acc[1] + left + right

    loads[2].wait()
    loads[3].wait()
    key_quad(0)
    key_quad(1)
    scatter(0)
    key_quad(2)
    put_slab(pairs, kst[...].T)
    loads[4].wait()
    query_quad(0)
    scatter(1)
    query_quad(1)
    gather(0)
    query_quad(2)
    gather(1)
    convolve()
    forward(0)
    forward(1)
    for gi in range(len(groups)):
        for copy in fw[gi]:
            copy.wait_recv()

    ks = fin[pairs]
    sumsq = jnp.zeros((nrows, LANES), F32)
    pick_row = lax.broadcasted_iota(jnp.int32, (LANES, LANES), 0)
    pick_lane = lax.broadcasted_iota(jnp.int32, (LANES, LANES), 1) // dh
    zero = jnp.zeros((), BF16)
    for p in range(pairs):
        pick = jnp.where(pick_row == 2 * p + pick_lane, 1.0, 0.0).astype(BF16)
        krep = mm(ks, pick).astype(BF16)
        sp = fin[p]
        lo = jnp.concatenate([jnp.where(lane_lo, sp, zero), jnp.where(lane_lo, krep, zero)], 1)
        hi = jnp.concatenate([jnp.where(lane_lo, zero, sp), jnp.where(lane_lo, zero, krep)], 1)
        both = mm(fq[2 * p], lo) + mm(fq[2 * p + 1], hi)
        attn = both[:, :LANES] / both[:, LANES:]
        att[:, LANES * p : LANES * (p + 1)] = attn
        sumsq = sumsq + attn * attn
    scale = lax.rsqrt(jnp.sum(sumsq, axis=1, keepdims=True) * (1.0 / width) + 1e-06)
    loads[5].wait()
    outs = []
    for r in range(rows_here):
        cut = slice(r * cols, (r + 1) * cols)
        mixed = (att[cut] * scale[cut] * gain_ref[...].reshape(1, width) + pos[cut]).astype(BF16)
        outv[cut] = (tok[cut].astype(F32) + mm(mixed, wo[...])).astype(BF16)
        copy = pltpu.make_async_copy(outv.at[cut], out_hbm.at[cut], out_sem.at[r])
        copy.start()
        outs.append(copy)

    @pl.when(me < n - 1)
    def _():
        to_next.wait_send()

    @pl.when(me > 0)
    def _():
        to_prev.wait_send()

    for copy in d2d:
        copy.wait_send()
    for gi in range(len(groups)):
        for copy in rs[gi] + ag[gi] + fw[gi]:
            copy.wait_send()
    for copy in outs:
        copy.wait()


def fused(n, tokens, w_query, w_key, w_value, w_out, omega, conv_kernel, norm_gain):
    rows_here, cols, width = tokens.shape
    heads, dh, nfeat = omega.shape
    nrows = rows_here * cols
    chips, half, slabs = n // 2, nfeat // 2, heads // 2 + 1
    piece = half // chips
    groups = ((0, 4), (4, slabs))
    dims = (n, rows_here, cols, width, heads, dh, nfeat, groups)
    any_spec = pl.BlockSpec(memory_space=pl.ANY)
    vmem_spec = pl.BlockSpec(memory_space=pltpu.VMEM)
    sem = pltpu.SemaphoreType.DMA
    ng = len(groups)
    flat = tokens.reshape(nrows, width)
    out = pl.pallas_call(
        functools.partial(kernel, dims),
        out_shape=jax.ShapeDtypeStruct((nrows, width), BF16),
        in_specs=[any_spec] * 6 + [vmem_spec] * 2,
        out_specs=any_spec,
        scratch_shapes=[
            pltpu.VMEM((nrows, width), BF16),
            pltpu.VMEM((width, width), BF16),
            pltpu.VMEM((width, width), BF16),
            pltpu.VMEM((width, width), BF16),
            pltpu.VMEM((width, width), BF16),
            pltpu.VMEM((heads, dh, nfeat), BF16),
            pltpu.VMEM((nrows, width), BF16),
            pltpu.VMEM((2, cols, width), BF16),
            pltpu.VMEM((heads, nrows, nfeat), BF16),
            pltpu.VMEM((nrows, width), F32),
            pltpu.VMEM((nrows, width), F32),
            pltpu.VMEM((nrows, width), BF16),
            pltpu.VMEM((slabs, nfeat, LANES), F32),
            pltpu.VMEM((LANES, nfeat), F32),
            pltpu.VMEM((slabs, half, LANES), BF16),
            pltpu.VMEM((slabs, half, LANES), BF16),
            pltpu.VMEM((chips, slabs, piece, LANES), BF16),
            pltpu.VMEM((chips, slabs, piece, LANES), BF16),
            pltpu.VMEM((slabs, nfeat, LANES), BF16),
            sem((6,)), sem((rows_here,)), sem((2,)), sem((2,)), sem((slabs,)), sem((slabs,)),
            sem((ng, chips)), sem((ng, chips)), sem((ng, chips)), sem((ng, chips)),
            sem((ng, chips)), sem((ng, chips)),
        ],
        compiler_params=pltpu.CompilerParams(
            collective_id=0, has_side_effects=True, vmem_limit_bytes=60 * 1024 * 1024
        ),
    )(flat, w_query, w_key, w_value, w_out, omega, conv_kernel, norm_gain)
    return out.reshape(tokens.shape)


def layer(n, *args):
    heads, dh, nfeat = args[5].shape
    width = args[0].shape[2]
    fits = (
        n % 2 == 0 and nfeat % (n * SUB) == 0 and 2 * dh == LANES and heads == 12
        and nfeat == 2 * LANES and width == heads * dh
    )
    return fused(n, *args) if fits else shards(*args)


def solution(mesh):
    return jax.shard_map(
        functools.partial(layer, mesh.shape["row"]),
        mesh=mesh,
        in_specs=(P(("parts", "row"), None, None), P(), P(), P(), P(), P(), P(), P()),
        out_specs=P(("parts", "row"), None, None),
        check_vma=False,
    )
```
